128 devices in a mesh: row: 16 (over y_lo, z, core), col: 8 (over y_hi, x).
Axes of the slice: x: 4, y: 4 (y_hi: 2, y_lo: 2; y = y_hi * 2 + y_lo), z: 4, core: 2. Of those that a mesh axis runs over, the one named last changes fastest.
Arguments:
- matrix: float32 [3456, 131072], P('row', 'col'), may hold values from -6 to 6
- range_basis: float32 [3456, 384], P('col', 'row'), may hold values from -0.125 to 0.125
Outputs:
- projected: float32 [384, 131072], P('row')
The draws below stay inside these ranges and needn't reach their ends.
All inputs are finite; a program needn't handle non-finite values.
Results may differ from the reference program's by a relative error of at most 0.000071.
Values sent between devices are 32-bit elements; how exact they have to be, the bound alone decides.
A program may use at most 128 MiB of HBM per device.

```python
import jax
import jax.numpy as jnp
from jax import lax

K = 384
M = 3456
N = 131072


def spiked(entries, own_key, source, target, shards_of, factor):
    owner, partner = [(jnp.arange(entries.shape[axis_at]) // (entries.shape[axis_at] // shards_of)).reshape([-1 if axis == axis_at else 1 for axis in range(entries.ndim)]) for axis_at in (source, target)]
    chosen = jax.random.permutation(own_key, shards_of)[partner]
    strong = (owner == chosen) | (owner == (partner + shards_of // 2) % shards_of)
    return jnp.where(strong, factor * entries, entries)


def levels(rng, shape, pieces, least, high):
    gain = 1.0
    for dim, parts in pieces:
        draws = jax.random.uniform(jax.random.fold_in(jax.random.fold_in(rng, 6), dim), (parts,), jnp.float32, least / len(pieces), high / len(pieces))
        gain = gain * jnp.repeat(jnp.exp(draws), shape[dim] // parts).reshape((-1,) + (1,) * (len(shape) - 1 - dim))
    return gain


def centred(stream_key, dims, width, bound, shards=(), kind=jnp.bfloat16):
    array = width * jax.random.normal(stream_key, dims, jnp.float32)
    if shards:
        array = array * levels(stream_key, dims, shards, -0.22, 0.18)
    return jnp.clip(array, -bound, bound).astype(kind)


def gaussian_with(key, shape, scale, reach, cuts, heavy, dtype=jnp.bfloat16):
    result = scale * jax.random.normal(key, shape, jnp.float32)
    if cuts:
        result = result * levels(key, shape, cuts, -0.22, 0.18)
    return jnp.clip(spiked(result, jax.random.fold_in(key, 3), *heavy), -reach, reach).astype(dtype)


def setup_inputs(seed: int = 0) -> dict:
    arg_keys = jax.random.split(jax.random.key(seed), 3)
    matrix = centred(arg_keys[0], (M, N), 1.0, 6.0, ((0, 16), (1, 8)), jnp.float32)
    range_basis = gaussian_with(arg_keys[1], (M, K), M ** -0.5, 0.125, ((0, 8), (1, 16)), (0, 1, 16, 2.0), jnp.float32)
    return {"matrix": matrix, "range_basis": range_basis}


def reference(matrix, range_basis):
    return lax.dot_general(range_basis, matrix, (((0,), (0,)), ((), ())), precision=lax.Precision.HIGHEST, preferred_element_type=jnp.float32)
```

```python
import functools

import jax
import jax.numpy as jnp
from jax import lax
from jax.experimental import pallas as pl
from jax.experimental.pallas import tpu as pltpu
from jax.sharding import PartitionSpec as P

MESH = pl.DeviceIdType.MESH
STEPS = 16
SLOTS = 8
F32 = jnp.float32
BF16 = jnp.bfloat16


def halves(value):
    high = value.astype(BF16)
    return high, (value - high.astype(F32)).astype(BF16)


def dot(left, right):
    return jnp.dot(left, right, preferred_element_type=F32)


def kernel(
    steps, a_ref, q_ref, o_ref,
    ab, qf, qhi, qlo, p, zr, yr, out,
    a_own, a_send, a_recv, q_send, q_recv, f_send, f_recv,
    z_send, z_recv, y_send, y_recv, c_send, c_recv, h_send, h_recv, x_send, x_recv, o_sem,
):
    rows, width = a_ref.shape
    basis = q_ref.shape[0]
    piece = width // steps
    half = piece // 2
    w = half // 2

    r, c = lax.axis_index("row"), lax.axis_index("col")
    k = lax.rem(r, 2)
    j = lax.div(r, 2)
    z = lax.rem(j, 4)
    ylo = lax.div(j, 4)
    x = lax.rem(c, 4)
    yhi = lax.div(c, 4)

    def row_of(ylo_, z_, k_):
        return (ylo_ * 4 + z_) * 2 + k_

    def wrap(v):
        return lax.rem(v + 8, 4)

    sibling = (row_of(ylo, z, 1 - k), c)
    z_next = [(row_of(ylo, wrap(z + 1), k), c), (row_of(ylo, wrap(z - 1), k), c)]
    y_pair = (row_of(1 - ylo, z, k), c)
    h_pair = (r, (1 - yhi) * 4 + x)
    x_next = [(r, yhi * 4 + wrap(x + 1)), (r, yhi * 4 + wrap(x - 1))]

    def remote(src, dst, send, recv, device):
        return pltpu.make_async_remote_copy(
            src_ref=src, dst_ref=dst, send_sem=send, recv_sem=recv,
            device_id=device, device_id_type=MESH,
        )

    def a_local(s):
        cols = pl.ds(pl.multiple_of(s * piece + k * half, 128), half)
        at = pl.ds(pl.multiple_of(k * rows, 8), rows)
        return pltpu.make_async_copy(a_ref.at[:, cols], ab.at[s, at], a_own.at[s])

    def a_swap(s):
        cols = pl.ds(pl.multiple_of(s * piece + (1 - k) * half, 128), half)
        at = pl.ds(pl.multiple_of(k * rows, 8), rows)
        return remote(a_ref.at[:, cols], ab.at[s, at], a_send.at[s], a_recv.at[s], sibling)

    def q_rows(q, k_):
        at = lax.rem(q, 4) * (4 * basis) + lax.div(q, 4) * (2 * basis) + k_ * basis
        return pl.ds(pl.multiple_of(at, 8), basis)

    def q_push(t):
        return remote(q_ref, qf.at[q_rows(j, k)], q_send.at[t], q_recv.at[j], (c * 2 + k, t))

    def q_here():
        return pltpu.make_async_copy(q_ref, qf.at[q_rows(j, k)], q_recv.at[j])

    def q_landed(q):
        return remote(q_ref, qf.at[q_rows(q, k)], q_send.at[q], q_recv.at[q], sibling)

    def q_forward(q):
        block = qf.at[q_rows(q, k)]
        return remote(block, block, f_send.at[q], f_recv.at[q], sibling)

    def z_rows(t, d):
        at = wrap(z - (1 - 2 * d) * (t + 1)) * (4 * basis)
        return pl.ds(pl.multiple_of(at, 8), 4 * basis)

    def z_copy(t, d, s):
        slot = lax.rem(s, SLOTS)
        u = s * 2 + d
        return remote(
            p.at[u, z_rows(t, d)], zr.at[t, u], z_send.at[t, d, slot], z_recv.at[t, d, slot], z_next[d]
        )

    def mine(ylo_, size, first):
        at = z * (4 * basis) + ylo_ * (2 * basis) + first * basis
        return pl.ds(pl.multiple_of(at, 8), size * basis)

    def y_copy(d, s):
        slot = lax.rem(s, SLOTS)
        u = s * 2 + d
        return remote(
            p.at[u, mine(1 - ylo, 2, 0)], yr.at[u], y_send.at[d, slot], y_recv.at[d, slot], y_pair
        )

    def part_cols(k_, d, s):
        at = c * width + s * piece + k_ * half + d * w
        return pl.ds(pl.multiple_of(at, 128), w)

    def c_copy(d, s):
        slot = lax.rem(s, SLOTS)
        return remote(
            p.at[s * 2 + d, mine(ylo, 1, 1 - k)], out.at[:, part_cols(k, d, s)],
            c_send.at[d, slot], c_recv.at[d, slot], sibling,
        )

    def cols_of(yhi_, x_, s):
        at = (yhi_ * 4 + x_) * width + s * piece
        return pl.ds(pl.multiple_of(at, 128), piece)

    def h_copy(s):
        slot = lax.rem(s, SLOTS)
        block = out.at[:, cols_of(yhi, x, s)]
        return remote(block, block, h_send.at[slot], h_recv.at[slot], h_pair)

    x_plan = [
        (yhi, x, 0), (yhi, x, 1), (yhi, wrap(x - 1), 0),
        (1 - yhi, x, 0), (1 - yhi, x, 1), (1 - yhi, wrap(x + 1), 1),
    ]

    def x_copy(m, s):
        slot = lax.rem(s, SLOTS)
        yhi_, x_, d = x_plan[m]
        block = out.at[:, cols_of(yhi_, x_, s)]
        return remote(block, block, x_send.at[m, slot], x_recv.at[m, slot], x_next[d])

    def flush(s, t):
        block = pl.ds(pl.multiple_of(t * width + s * piece, 128), piece)
        return pltpu.make_async_copy(out.at[:, block], o_ref.at[:, block], o_sem.at[t, lax.rem(s, SLOTS)])

    @pl.loop(0, steps)
    def _(s):
        a_local(s).start()

    at_home = c == j
    barrier = pltpu.get_barrier_semaphore()
    for device in [sibling, *z_next, y_pair, h_pair, *x_next]:
        pl.semaphore_signal(barrier, inc=1, device_id=device, device_id_type=MESH)

    @pl.loop(0, 8)
    def _(q):
        @pl.when(jnp.logical_not(jnp.logical_and(at_home, q == j)))
        def _():
            pl.semaphore_signal(barrier, inc=1, device_id=(2 * q + k, j), device_id_type=MESH)

    pl.semaphore_wait(barrier, 15 - jnp.where(at_home, 1, 0))

    @pl.loop(0, 8)
    def _(t):
        home = jnp.logical_and(at_home, t == c)

        @pl.when(jnp.logical_not(home))
        def _():
            q_push(t).start()

        @pl.when(home)
        def _():
            q_here().start()

    @pl.loop(0, steps)
    def _(s):
        a_swap(s).start()

    @pl.loop(0, 8)
    def _(q):
        q_landed(q).wait_recv()
        q_forward(q).start()

    @pl.loop(0, 8)
    def _(q):
        q_forward(q).wait_recv()

    high, low = halves(qf[...])
    qhi[...] = high
    qlo[...] = low

    def compute(s):
        a_local(s).wait()
        a_swap(s).wait_recv()
        for d in range(2):
            a_high, a_low = halves(ab[s, :, d * w : (d + 1) * w])
            p[s * 2 + d] = dot(qhi[...], a_low) + dot(qlo[...], a_high) + dot(qhi[...], a_high)
        for d in range(2):
            z_copy(0, d, s).start()

    def z_add(t, d, s):
        z_copy(t - 1, d, s).wait_recv()
        u = s * 2 + d
        at = z_rows(t, d)
        p[u, at] = p[u, at] + zr[t - 1, u]

    def live(i, lag, body):
        @pl.when(jnp.logical_and(i >= lag, i < steps + lag))
        def _():
            body(i - lag)

    def z_last(s):
        for d in range(2):
            z_add(3, d, s)
            y_copy(d, s).start()

    def z_step(t):
        def body(s):
            for d in range(2):
                z_add(t, d, s)
                z_copy(t, d, s).start()
        return body

    def y_last(s):
        for d in range(2):
            y_copy(d, s).wait_recv()
            u = s * 2 + d
            own, other = mine(ylo, 1, k), mine(ylo, 1, 1 - k)
            y_own = pl.ds(pl.multiple_of(k * basis, 8), basis)
            y_other = pl.ds(pl.multiple_of((1 - k) * basis, 8), basis)
            p[u, other] = p[u, other] + yr[u, y_other]
            c_copy(d, s).start()
            out[:, part_cols(k, d, s)] = p[u, own] + yr[u, y_own]

    def spread(s):
        for d in range(2):
            c_copy(d, s).wait_recv()
        h_copy(s).start()
        x_copy(0, s).start()
        x_copy(1, s).start()

    def spread_far(s):
        h_copy(s).wait_recv()
        x_copy(3, s).start()
        x_copy(4, s).start()

    def forward(m, first):
        def body(s):
            x_copy(first, s).wait_recv()
            x_copy(m, s).start()
        return body

    def retire(s):
        for d in range(2):
            for t in range(3):
                z_copy(t, d, s).wait_send()
            y_copy(d, s).wait_send()
            c_copy(d, s).wait_send()
        h_copy(s).wait_send()
        for m in (1, 2, 3, 5):
            x_copy(m, s).wait_recv()
        for m in range(6):
            x_copy(m, s).wait_send()

        @pl.when(s >= SLOTS)
        def _():
            @pl.loop(0, 8)
            def _(t):
                flush(s - SLOTS, t).wait()

        @pl.loop(0, 8)
        def _(t):
            flush(s, t).start()

    compute(0)

    @pl.loop(0, steps + 6)
    def _(i):
        live(i, 3, z_last)
        live(i, 2, z_step(2))
        live(i, 1, z_step(1))

        @pl.when(i + 1 < steps)
        def _():
            compute(i + 1)

        live(i, 3, y_last)
        live(i, 4, spread_far)
        live(i, 4, forward(2, 0))
        live(i, 5, forward(5, 4))
        live(i, 3, spread)
        live(i, 6, retire)

    @pl.loop(steps - SLOTS if steps > SLOTS else 0, steps)
    def _(s):
        @pl.loop(0, 8)
        def _(t):
            flush(s, t).wait()

    @pl.loop(0, steps)
    def _(s):
        a_swap(s).wait_send()

    @pl.loop(0, 8)
    def _(t):
        q_forward(t).wait_send()

        @pl.when(jnp.logical_not(jnp.logical_and(at_home, t == c)))
        def _():
            q_push(t).wait_send()


def per_device(steps, matrix, range_basis):
    rows, width = matrix.shape
    depth, basis = range_basis.shape
    w = width // steps // 4
    dma = pltpu.SemaphoreType.DMA
    return pl.pallas_call(
        functools.partial(kernel, steps),
        out_shape=jax.ShapeDtypeStruct((basis, 8 * width), F32),
        in_specs=[pl.BlockSpec(memory_space=pl.ANY)] * 2,
        out_specs=pl.BlockSpec(memory_space=pl.ANY),
        scratch_shapes=[
            pltpu.VMEM((steps, 2 * rows, 2 * w), F32),
            pltpu.VMEM((16 * basis, depth), F32),
            pltpu.VMEM((16 * basis, depth), BF16),
            pltpu.VMEM((16 * basis, depth), BF16),
            pltpu.VMEM((2 * steps, 16 * basis, w), F32),
            pltpu.VMEM((3, 2 * steps, 4 * basis, w), F32),
            pltpu.VMEM((2 * steps, 2 * basis, w), F32),
            pltpu.VMEM((basis, 8 * width), F32),
            dma((steps,)), dma((steps,)), dma((steps,)),
            dma((8,)), dma((8,)), dma((8,)), dma((8,)),
            dma((3, 2, SLOTS)), dma((3, 2, SLOTS)),
            dma((2, SLOTS)), dma((2, SLOTS)), dma((2, SLOTS)), dma((2, SLOTS)),
            dma((SLOTS,)), dma((SLOTS,)), dma((6, SLOTS)), dma((6, SLOTS)), dma((8, SLOTS)),
        ],
        compiler_params=pltpu.CompilerParams(
            collective_id=0, has_side_effects=True, vmem_limit_bytes=60 * 1024 * 1024
        ),
    )(matrix, range_basis.T)


def solution(mesh):
    in_specs = (P("row", "col"), P("col", "row"))
    out_specs = P("row", None)
    return jax.shard_map(
        functools.partial(per_device, STEPS), mesh=mesh, in_specs=in_specs, out_specs=out_specs, check_vma=False
    )
```

```python
import functools

import jax
import jax.numpy as jnp
from jax import lax
from jax.experimental import pallas as pl
from jax.experimental.pallas import tpu as pltpu
from jax.sharding import PartitionSpec as P

MESH = pl.DeviceIdType.MESH
UNITS = 32
SLOTS = 16
AHEAD = 6
F32 = jnp.float32
BF16 = jnp.bfloat16
Z_LAGS = (-2, 2, 4, 6)
Y_LAG, SPREAD_LAG, FAR_LAG, NEAR_ON_LAG, FAR_ON_LAG, RETIRE_LAG = 7, 8, 9, 10, 12, 14


def halves(value):
    high = value.astype(BF16)
    return high, (value - high.astype(F32)).astype(BF16)


def dot(left, right):
    return jnp.dot(left, right, preferred_element_type=F32)


def kernel(
    units, a_ref, q_ref, out,
    ab, qv, qf, qhi, qlo, p, zr, yr,
    a_own, a_send, a_recv, q_own, q_send, q_recv, f_send, f_recv,
    z_send, z_recv, y_send, y_recv, c_send, c_recv, h_send, h_recv, x_send, x_recv,
):
    rows, width = a_ref.shape
    basis = q_ref.shape[0]
    pair = width // units
    w = pair // 2

    r, c = lax.axis_index("row"), lax.axis_index("col")
    k = lax.rem(r, 2)
    j = lax.div(r, 2)
    z = lax.rem(j, 4)
    ylo = lax.div(j, 4)
    x = lax.rem(c, 4)
    yhi = lax.div(c, 4)

    def row_of(ylo_, z_, k_):
        return (ylo_ * 4 + z_) * 2 + k_

    def wrap(v):
        return lax.rem(v + 8, 4)

    sibling = (row_of(ylo, z, 1 - k), c)
    z_next = [(row_of(ylo, wrap(z + 1), k), c), (row_of(ylo, wrap(z - 1), k), c)]
    y_pair = (row_of(1 - ylo, z, k), c)
    h_pair = [(row_of(1 - ylo, z, k_), (1 - yhi) * 4 + x) for k_ in range(2)]
    x_next = [(r, yhi * 4 + wrap(x + 1)), (r, yhi * 4 + wrap(x - 1))]

    def remote(src, dst, send, recv, device):
        return pltpu.make_async_remote_copy(
            src_ref=src, dst_ref=dst, send_sem=send, recv_sem=recv,
            device_id=device, device_id_type=MESH,
        )

    def slot(u):
        return lax.rem(u, SLOTS)

    def a_local(u):
        cols = pl.ds(pl.multiple_of(u * pair + k * w, 128), w)
        at = pl.ds(pl.multiple_of(k * rows, 8), rows)
        return pltpu.make_async_copy(a_ref.at[:, cols], ab.at[u, at], a_own.at[slot(u)])

    def a_swap(u):
        cols = pl.ds(pl.multiple_of(u * pair + (1 - k) * w, 128), w)
        at = pl.ds(pl.multiple_of(k * rows, 8), rows)
        return remote(a_ref.at[:, cols], ab.at[u, at], a_send.at[slot(u)], a_recv.at[slot(u)], sibling)

    def q_rows(q, k_):
        at = lax.rem(q, 4) * (4 * basis) + lax.div(q, 4) * (2 * basis) + k_ * basis
        return pl.ds(pl.multiple_of(at, 8), basis)

    def q_push(t):
        return remote(qv, qf.at[q_rows(j, k)], q_send.at[t], q_recv.at[j], (c * 2 + k, t))

    def q_here():
        return pltpu.make_async_copy(q_ref, qf.at[q_rows(j, k)], q_recv.at[j])

    def q_landed(q):
        return remote(qv, qf.at[q_rows(q, k)], q_send.at[q], q_recv.at[q], sibling)

    def q_forward(q):
        block = qf.at[q_rows(q, k)]
        return remote(block, block, f_send.at[q], f_recv.at[q], sibling)

    def z_rows(t, d):
        at = wrap(z - (1 - 2 * d) * (t + 1)) * (4 * basis)
        return pl.ds(pl.multiple_of(at, 8), 4 * basis)

    def z_copy(t, d, u):
        return remote(
            p.at[u, z_rows(t, d)], zr.at[t, u], z_send.at[t, slot(u)], z_recv.at[t, slot(u)], z_next[d]
        )

    def y_copy(u):
        return remote(p.at[u, z_rows(3, 0)], yr.at[u], y_send.at[slot(u)], y_recv.at[slot(u)], y_pair)

    def y_rows(ylo_, k_):
        return pl.ds(pl.multiple_of(ylo_ * (2 * basis) + k_ * basis, 8), basis)

    def part_cols(u):
        at = c * width + u * pair + k * w
        return pl.ds(pl.multiple_of(at, 128), w)

    def c_copy(u):
        return remote(
            yr.at[u, y_rows(ylo, 1 - k)], out.at[:, part_cols(u)],
            c_send.at[slot(u)], c_recv.at[slot(u)], sibling,
        )

    def h_copy(k_, u):
        return remote(
            yr.at[u, y_rows(1 - ylo, k_)], out.at[:, part_cols(u)],
            h_send.at[k_, slot(u)], h_recv.at[k, slot(u)], h_pair[k_],
        )

    def h_landed(k_, u):
        return remote(
            yr.at[u, y_rows(1 - ylo, k_)], out.at[:, part_cols(u)],
            h_send.at[k_, slot(u)], h_recv.at[k_, slot(u)], h_pair[k_],
        )

    x_plan = [
        (yhi, x, 0), (yhi, x, 1), (yhi, wrap(x - 1), 0),
        (1 - yhi, x, 0), (1 - yhi, x, 1), (1 - yhi, wrap(x + 1), 1),
    ]

    def x_copy(m, u):
        yhi_, x_, d = x_plan[m]
        at = (yhi_ * 4 + x_) * width + u * pair
        block = out.at[:, pl.ds(pl.multiple_of(at, 128), pair)]
        return remote(block, block, x_send.at[m, slot(u)], x_recv.at[m, slot(u)], x_next[d])

    q_mine = pltpu.make_async_copy(q_ref, qv, q_own)
    q_mine.start()

    @pl.loop(0, AHEAD)
    def _(u):
        a_local(u).start()

    at_home = c == j
    barrier = pltpu.get_barrier_semaphore()
    for device in [sibling, *z_next, y_pair, *h_pair, *x_next]:
        pl.semaphore_signal(barrier, inc=1, device_id=device, device_id_type=MESH)

    @pl.loop(0, 8)
    def _(q):
        @pl.when(jnp.logical_not(jnp.logical_and(at_home, q == j)))
        def _():
            pl.semaphore_signal(barrier, inc=1, device_id=(2 * q + k, j), device_id_type=MESH)

    q_mine.wait()
    pl.semaphore_wait(barrier, 16 - jnp.where(at_home, 1, 0))

    @pl.loop(0, 8)
    def _(t):
        home = jnp.logical_and(at_home, t == c)

        @pl.when(jnp.logical_not(home))
        def _():
            q_push(t).start()

        @pl.when(home)
        def _():
            q_here().start()

    @pl.loop(0, 4)
    def _(u):
        a_swap(u).start()

    @pl.loop(0, 8)
    def _(q):
        q_landed(q).wait_recv()
        q_forward(q).start()

    @pl.loop(4, AHEAD)
    def _(u):
        a_swap(u).start()

    @pl.loop(0, 8)
    def _(q):
        q_forward(q).wait_recv()

    high, low = halves(qf[...])
    qhi[...] = high
    qlo[...] = low

    def compute(d, u):
        a_local(u).wait()
        a_swap(u).wait_recv()
        a_high, a_low = halves(ab[u])
        p[u] = dot(qhi[...], a_low) + dot(qlo[...], a_high) + dot(qhi[...], a_high)
        z_copy(0, d, u).start()

    def fetch(d, u):
        @pl.when(u >= SLOTS)
        def _():
            a_swap(u - SLOTS).wait_send()

        a_local(u).start()
        a_swap(u).start()

    def z_step(t):
        def body(d, u):
            z_copy(t - 1, d, u).wait_recv()
            at = z_rows(t, d)
            p[u, at] = p[u, at] + zr[t - 1, u]
            if t < 3:
                z_copy(t, d, u).start()
            else:
                y_copy(u).start()
        return body

    def y_last(d, u):
        y_copy(u).wait_recv()
        total = p[u, z_rows(3, 0)] + yr[u]
        yr[u] = total
        c_copy(u).start()
        for k_ in range(2):
            h_copy(k_, u).start()
        out[:, part_cols(u)] = yr[u, y_rows(ylo, k)]

    def spread(d, u):
        c_copy(u).wait_recv()
        x_copy(0, u).start()
        x_copy(1, u).start()

    def spread_far(d, u):
        for k_ in range(2):
            h_landed(k_, u).wait_recv()
        x_copy(3, u).start()
        x_copy(4, u).start()

    def forward(m, first):
        def body(d, u):
            x_copy(first, u).wait_recv()
            x_copy(m, u).start()
        return body

    def retire(d, u):
        for t in range(3):
            z_copy(t, d, u).wait_send()
        y_copy(u).wait_send()
        c_copy(u).wait_send()
        for k_ in range(2):
            h_copy(k_, u).wait_send()
        for m in (1, 2, 3, 5):
            x_copy(m, u).wait_recv()
        for m in range(6):
            x_copy(m, u).wait_send()

    for d in range(2):
        compute(d, d)

    @pl.loop(0, (units + RETIRE_LAG) // 2)
    def _(i):
        for d in range(2):
            def live(lag, body):
                u = 2 * i + d - lag

                @pl.when(jnp.logical_and(u >= max(-lag, 0), u < units))
                def _():
                    body((d - lag) % 2, u)

            live(RETIRE_LAG, retire)
            live(-AHEAD, fetch)
            for t in (3, 2, 1):
                live(Z_LAGS[t], z_step(t))
            live(Z_LAGS[0], compute)
            live(SPREAD_LAG, spread)
            live(FAR_LAG, spread_far)
            live(NEAR_ON_LAG, forward(2, 0))
            live(FAR_ON_LAG, forward(5, 4))
            live(Y_LAG, y_last)

    @pl.loop(units - SLOTS, units)
    def _(u):
        a_swap(u).wait_send()

    @pl.loop(0, 8)
    def _(t):
        q_forward(t).wait_send()

        @pl.when(jnp.logical_not(jnp.logical_and(at_home, t == c)))
        def _():
            q_push(t).wait_send()


def per_device(units, matrix, range_basis):
    rows, width = matrix.shape
    depth, basis = range_basis.shape
    w = width // units // 2
    dma = pltpu.SemaphoreType.DMA
    ring = dma((SLOTS,))
    return pl.pallas_call(
        functools.partial(kernel, units),
        out_shape=pltpu.VMEM((basis, 8 * width), F32),
        in_specs=[pl.BlockSpec(memory_space=pl.ANY)] * 2,
        out_specs=pl.BlockSpec(memory_space=pltpu.VMEM),
        scratch_shapes=[
            pltpu.VMEM((units, 2 * rows, w), F32),
            pltpu.VMEM((basis, depth), F32),
            pltpu.VMEM((16 * basis, depth), F32),
            pltpu.VMEM((16 * basis, depth), BF16),
            pltpu.VMEM((16 * basis, depth), BF16),
            pltpu.VMEM((units, 16 * basis, w), F32),
            pltpu.VMEM((3, units, 4 * basis, w), F32),
            pltpu.VMEM((units, 4 * basis, w), F32),
            ring, ring, ring,
            dma, dma((8,)), dma((8,)), dma((8,)), dma((8,)),
            dma((3, SLOTS)), dma((3, SLOTS)), ring, ring, ring, ring,
            dma((2, SLOTS)), dma((2, SLOTS)), dma((6, SLOTS)), dma((6, SLOTS)),
        ],
        compiler_params=pltpu.CompilerParams(
            collective_id=0, has_side_effects=True, vmem_limit_bytes=46 * 1024 * 1024
        ),
    )(matrix, range_basis.T)


def solution(mesh):
    in_specs = (P("row", "col"), P("col", "row"))
    out_specs = P("row", None)
    return jax.shard_map(
        functools.partial(per_device, UNITS), mesh=mesh, in_specs=in_specs, out_specs=out_specs, check_vma=False
    )
```

```python
import functools

import jax
import jax.numpy as jnp
from jax import lax
from jax.experimental import pallas as pl
from jax.experimental.pallas import tpu as pltpu
from jax.sharding import PartitionSpec as P

MESH = pl.DeviceIdType.MESH
UNITS = 64
SHORT, LONG = 8, 16
AHEAD = 6
F32 = jnp.float32
BF16 = jnp.bfloat16
STAGES = (
    ("z1", 0),
    ("far_on", 12),
    ("compute", -3),
    ("z0", -3),
    ("z3", 5),
    ("spread", 8),
    ("retire", 14),
    ("fetch", -AHEAD),
    ("y", 7),
    ("far", 9),
    ("z2", 2),
    ("near_on", 10),
)


def halves(value):
    high = value.astype(BF16)
    return high, (value - high.astype(F32)).astype(BF16)


def dot(left, right):
    return jnp.dot(left, right, preferred_element_type=F32)


def kernel(
    units, a_ref, q_ref, out,
    ab, qv, qf, qhi, qlo, p, zr, yr,
    a_own, a_send, a_recv, q_own, q_send, q_recv, f_send, f_recv,
    sent, z_recv, y_recv, c_recv, h_recv, x_recv, x_rest,
):
    rows, width = a_ref.shape
    basis = q_ref.shape[0]
    pair = width // units
    w = pair // 2

    r, c = lax.axis_index("row"), lax.axis_index("col")
    k = lax.rem(r, 2)
    j = lax.div(r, 2)
    z = lax.rem(j, 4)
    ylo = lax.div(j, 4)
    x = lax.rem(c, 4)
    yhi = lax.div(c, 4)

    def row_of(ylo_, z_, k_):
        return (ylo_ * 4 + z_) * 2 + k_

    def wrap(v):
        return lax.rem(v + 8, 4)

    sibling = (row_of(ylo, z, 1 - k), c)
    z_next = [(row_of(ylo, wrap(z + 1), k), c), (row_of(ylo, wrap(z - 1), k), c)]
    y_pair = (row_of(1 - ylo, z, k), c)
    h_pair = [(row_of(1 - ylo, z, k_), (1 - yhi) * 4 + x) for k_ in range(2)]
    x_next = [(r, yhi * 4 + wrap(x + 1)), (r, yhi * 4 + wrap(x - 1))]

    def remote(src, dst, send, recv, device):
        return pltpu.make_async_remote_copy(
            src_ref=src, dst_ref=dst, send_sem=send, recv_sem=recv,
            device_id=device, device_id_type=MESH,
        )

    def short(u):
        return lax.rem(u, SHORT)

    def long(u):
        return lax.rem(u, LONG)

    def a_local(u):
        cols = pl.ds(pl.multiple_of(u * pair + k * w, 128), w)
        at = pl.ds(pl.multiple_of(k * rows, 8), rows)
        return pltpu.make_async_copy(a_ref.at[:, cols], ab.at[u, at], a_own.at[short(u)])

    def a_swap(u):
        cols = pl.ds(pl.multiple_of(u * pair + (1 - k) * w, 128), w)
        at = pl.ds(pl.multiple_of(k * rows, 8), rows)
        return remote(a_ref.at[:, cols], ab.at[u, at], a_send.at[long(u)], a_recv.at[long(u)], sibling)

    def q_rows(q, k_):
        at = lax.rem(q, 4) * (4 * basis) + lax.div(q, 4) * (2 * basis) + k_ * basis
        return pl.ds(pl.multiple_of(at, 8), basis)

    def q_push(t):
        return remote(qv, qf.at[q_rows(j, k)], q_send, q_recv.at[j], (c * 2 + k, t))

    def q_here():
        return pltpu.make_async_copy(q_ref, qf.at[q_rows(j, k)], q_recv.at[j])

    def q_landed(q):
        return remote(qv, qf.at[q_rows(q, k)], q_send, q_recv.at[q], sibling)

    def q_forward(q):
        block = qf.at[q_rows(q, k)]
        return remote(block, block, f_send, f_recv, sibling)

    def q_amount(blocks, sem):
        part = qf.at[pl.ds(0, blocks * basis)]
        return pltpu.make_async_copy(part, part, sem)

    def z_rows(t, d):
        at = wrap(z - (1 - 2 * d) * (t + 1)) * (4 * basis)
        return pl.ds(pl.multiple_of(at, 8), 4 * basis)

    def z_copy(t, d, u):
        return remote(
            p.at[u, z_rows(t, d)], zr.at[t, u], sent.at[long(u)], z_recv.at[t, short(u)], z_next[d]
        )

    def y_copy(u):
        return remote(p.at[u, z_rows(3, 0)], yr.at[u], sent.at[long(u)], y_recv.at[short(u)], y_pair)

    def y_rows(ylo_, k_):
        return pl.ds(pl.multiple_of(ylo_ * (2 * basis) + k_ * basis, 8), basis)

    def part_cols(u):
        at = c * width + u * pair + k * w
        return pl.ds(pl.multiple_of(at, 128), w)

    def c_copy(u):
        return remote(
            yr.at[u, y_rows(ylo, 1 - k)], out.at[:, part_cols(u)],
            sent.at[long(u)], c_recv.at[short(u)], sibling,
        )

    def h_copy(k_, u):
        return remote(
            yr.at[u, y_rows(1 - ylo, k_)], out.at[:, part_cols(u)],
            sent.at[long(u)], h_recv.at[short(u)], h_pair[k_],
        )

    def block_of(yhi_, x_, u):
        at = (yhi_ * 4 + x_) * width + u * pair
        return out.at[:, pl.ds(pl.multiple_of(at, 128), pair)]

    def h_landed(u):
        block = block_of(1 - yhi, x, u)
        return remote(block, block, sent.at[long(u)], h_recv.at[short(u)], sibling)

    x_plan = [
        (yhi, x, 0), (yhi, x, 1), (yhi, wrap(x - 1), 0),
        (1 - yhi, x, 0), (1 - yhi, x, 1), (1 - yhi, wrap(x + 1), 1),
    ]

    def x_copy(m, u):
        yhi_, x_, d = x_plan[m]
        block = block_of(yhi_, x_, u)
        recv = {0: x_recv.at[0, short(u)], 4: x_recv.at[1, short(u)]}.get(m, x_rest.at[long(u)])
        return remote(block, block, sent.at[long(u)], recv, x_next[d])

    def amount(strips):
        return out.at[:, pl.ds(0, strips * w)]

    def retired(u):
        return pltpu.make_async_copy(amount(31), amount(31), sent.at[long(u)])

    def rest_landed(u):
        return pltpu.make_async_copy(amount(8), amount(8), x_rest.at[long(u)])

    q_mine = pltpu.make_async_copy(q_ref, qv, q_own)
    q_mine.start()

    @pl.loop(0, AHEAD)
    def _(u):
        a_local(u).start()

    at_home = c == j
    barrier = pltpu.get_barrier_semaphore()
    for device in [sibling, *z_next, y_pair, *h_pair, *x_next]:
        pl.semaphore_signal(barrier, inc=1, device_id=device, device_id_type=MESH)

    @pl.loop(0, 8)
    def _(q):
        @pl.when(jnp.logical_not(jnp.logical_and(at_home, q == j)))
        def _():
            pl.semaphore_signal(barrier, inc=1, device_id=(2 * q + k, j), device_id_type=MESH)

    q_mine.wait()
    pl.semaphore_wait(barrier, 16 - jnp.where(at_home, 1, 0))

    @pl.loop(0, 8)
    def _(t):
        home = jnp.logical_and(at_home, t == c)

        @pl.when(jnp.logical_not(home))
        def _():
            q_push(t).start()

        @pl.when(home)
        def _():
            q_here().start()

    @pl.loop(0, 4)
    def _(u):
        a_swap(u).start()

    @pl.loop(0, 8)
    def _(q):
        q_landed(q).wait_recv()
        q_forward(q).start()

    @pl.loop(4, AHEAD)
    def _(u):
        a_swap(u).start()

    q_amount(8, f_recv).wait()
    high, low = halves(qf[...])
    qhi[...] = high
    qlo[...] = low

    def compute(d, u):
        a_local(u).wait()
        a_swap(u).wait_recv()
        a_high, a_low = halves(ab[u])
        p[u] = dot(qhi[...], a_low) + dot(qlo[...], a_high) + dot(qhi[...], a_high)

    def z_first(d, u):
        z_copy(0, d, u).start()

    def fetch(d, u):
        @pl.when(u >= LONG)
        def _():
            a_swap(u - LONG).wait_send()

        a_local(u).start()
        a_swap(u).start()

    def z_step(t):
        def body(d, u):
            z_copy(t - 1, d, u).wait_recv()
            at = z_rows(t, d)
            p[u, at] = p[u, at] + zr[t - 1, u]
            if t < 3:
                z_copy(t, d, u).start()
            else:
                y_copy(u).start()
        return body

    def y_last(d, u):
        y_copy(u).wait_recv()
        total = p[u, z_rows(3, 0)] + yr[u]
        yr[u] = total
        c_copy(u).start()
        for k_ in range(2):
            h_copy(k_, u).start()
        out[:, part_cols(u)] = yr[u, y_rows(ylo, k)]

    def spread(d, u):
        c_copy(u).wait_recv()
        x_copy(0, u).start()
        x_copy(1, u).start()

    def spread_far(d, u):
        h_landed(u).wait_recv()
        x_copy(3, u).start()
        x_copy(4, u).start()

    def forward(m, first):
        def body(d, u):
            x_copy(first, u).wait_recv()
            x_copy(m, u).start()
        return body

    def retire(d, u):
        rest_landed(u).wait()
        retired(u).wait()

    bodies = {
        "retire": retire, "fetch": fetch, "z3": z_step(3), "z2": z_step(2), "z1": z_step(1), "z0": z_first,
        "compute": compute, "y": y_last, "spread": spread, "far": spread_far,
        "near_on": forward(2, 0), "far_on": forward(5, 4),
    }
    lags = dict(STAGES)
    for u in range(-min(lags["compute"], lags["z0"])):
        for name in ("compute", "z0"):
            if u < -lags[name]:
                bodies[name](u % 2, u)

    @pl.loop(0, (units + max(lags.values()) + 1) // 2)
    def _(i):
        for d in range(2):
            for name, lag in STAGES:
                u = 2 * i + d - lag

                @pl.when(jnp.logical_and(u >= max(-lag, 0), u < units))
                def _():
                    bodies[name]((d - lag) % 2, u)

    @pl.loop(units - LONG, units)
    def _(u):
        a_swap(u).wait_send()

    q_amount(8, f_send).wait()

    @pl.when(at_home)
    def _():
        q_amount(7, q_send).wait()

    @pl.when(jnp.logical_not(at_home))
    def _():
        q_amount(8, q_send).wait()


def per_device(units, matrix, range_basis):
    rows, width = matrix.shape
    depth, basis = range_basis.shape
    w = width // units // 2
    dma = pltpu.SemaphoreType.DMA
    short, long = dma((SHORT,)), dma((LONG,))
    return pl.pallas_call(
        functools.partial(kernel, units),
        out_shape=pltpu.VMEM((basis, 8 * width), F32),
        in_specs=[pl.BlockSpec(memory_space=pl.ANY)] * 2,
        out_specs=pl.BlockSpec(memory_space=pltpu.VMEM),
        scratch_shapes=[
            pltpu.VMEM((units, 2 * rows, w), F32),
            pltpu.VMEM((basis, depth), F32),
            pltpu.VMEM((16 * basis, depth), F32),
            pltpu.VMEM((16 * basis, depth), BF16),
            pltpu.VMEM((16 * basis, depth), BF16),
            pltpu.VMEM((units, 16 * basis, w), F32),
            pltpu.VMEM((3, units, 4 * basis, w), F32),
            pltpu.VMEM((units, 4 * basis, w), F32),
            short, long, long, dma, dma, dma((8,)), dma, dma,
            long, dma((3, SHORT)), short, short, short, dma((2, SHORT)), long,
        ],
        compiler_params=pltpu.CompilerParams(
            collective_id=0, has_side_effects=True, vmem_limit_bytes=46 * 1024 * 1024
        ),
    )(matrix, range_basis.T)


def solution(mesh):
    in_specs = (P("row", "col"), P("col", "row"))
    out_specs = P("row", None)
    return jax.shard_map(
        functools.partial(per_device, UNITS), mesh=mesh, in_specs=in_specs, out_specs=out_specs, check_vma=False
    )
```

```python
import functools

import jax
import jax.numpy as jnp
from jax import lax
from jax.experimental import pallas as pl
from jax.experimental.pallas import tpu as pltpu
from jax.sharding import PartitionSpec as P

MESH = pl.DeviceIdType.MESH
UNITS = 64
SHORT, LONG = 10, 16
AHEAD = 6
F32 = jnp.float32
BF16 = jnp.bfloat16
STAGES = (
    ("spread", 7), ("far_on", 11), ("z1", 1), ("y", 6), ("compute", -2), ("z0", -2), ("far", 8), ("near_on", 9),
    ("z2", 3), ("retire", 13), ("fetch", -AHEAD),
)


def halves(value):
    high = value.astype(BF16)
    return high, (value - high.astype(F32)).astype(BF16)


def dot(left, right):
    return jnp.dot(left, right, preferred_element_type=F32)


def kernel(
    units, a_ref, q_ref, out,
    ab, qv, qf, qhi, qlo, p, zr, yr,
    a_own, a_send, a_recv, q_own, q_send, q_recv, f_send, f_recv,
    sent, z_recv, y_recv, c_recv, h_recv, x_recv, x_rest,
):
    rows, width = a_ref.shape
    basis = q_ref.shape[0]
    pair = width // units
    w = pair // 2

    r, c = lax.axis_index("row"), lax.axis_index("col")
    k = lax.rem(r, 2)
    j = lax.div(r, 2)
    z = lax.rem(j, 4)
    ylo = lax.div(j, 4)
    x = lax.rem(c, 4)
    yhi = lax.div(c, 4)

    def row_of(ylo_, z_, k_):
        return (ylo_ * 4 + z_) * 2 + k_

    def wrap(v):
        return lax.rem(v + 8, 4)

    sibling = (row_of(ylo, z, 1 - k), c)
    z_next = [(row_of(ylo, wrap(z + 1), k), c), (row_of(ylo, wrap(z - 1), k), c)]
    y_pair = (row_of(1 - ylo, z, k), c)
    h_pair = [(row_of(1 - ylo, z, k_), (1 - yhi) * 4 + x) for k_ in range(2)]
    x_next = [(r, yhi * 4 + wrap(x + 1)), (r, yhi * 4 + wrap(x - 1))]

    def remote(src, dst, send, recv, device):
        return pltpu.make_async_remote_copy(
            src_ref=src, dst_ref=dst, send_sem=send, recv_sem=recv,
            device_id=device, device_id_type=MESH,
        )

    def short(u):
        return lax.rem(u, SHORT)

    def long(u):
        return lax.rem(u, LONG)

    def a_local(u):
        cols = pl.ds(pl.multiple_of(u * pair + k * w, 128), w)
        at = pl.ds(pl.multiple_of(k * rows, 8), rows)
        return pltpu.make_async_copy(a_ref.at[:, cols], ab.at[u, at], a_own.at[short(u)])

    def a_swap(u):
        cols = pl.ds(pl.multiple_of(u * pair + (1 - k) * w, 128), w)
        at = pl.ds(pl.multiple_of(k * rows, 8), rows)
        return remote(a_ref.at[:, cols], ab.at[u, at], a_send.at[long(u)], a_recv.at[long(u)], sibling)

    def q_rows(q, k_):
        at = lax.rem(q, 4) * (4 * basis) + lax.div(q, 4) * (2 * basis) + k_ * basis
        return pl.ds(pl.multiple_of(at, 8), basis)

    def q_push(t):
        return remote(qv, qf.at[q_rows(j, k)], q_send, q_recv.at[j], (c * 2 + k, t))

    def q_here():
        return pltpu.make_async_copy(q_ref, qf.at[q_rows(j, k)], q_recv.at[j])

    def q_landed(q):
        return remote(qv, qf.at[q_rows(q, k)], q_send, q_recv.at[q], sibling)

    def q_forward(q):
        block = qf.at[q_rows(q, k)]
        return remote(block, block, f_send, f_recv, sibling)

    def q_amount(blocks, sem):
        part = qf.at[pl.ds(0, blocks * basis)]
        return pltpu.make_async_copy(part, part, sem)

    def z_rows(away):
        return pl.ds(pl.multiple_of(wrap(z + away) * (4 * basis), 8), 4 * basis)

    def z_copy(kind, d, u):
        ahead = 1 - 2 * d
        away, way = ((2 * ahead, d), (ahead, d), (-ahead, 1 - d))[kind]
        return remote(
            p.at[u, z_rows(away)], zr.at[kind, u], sent.at[long(u)], z_recv.at[kind, short(u)], z_next[way]
        )

    def y_copy(u):
        return remote(p.at[u, z_rows(0)], yr.at[u], sent.at[long(u)], y_recv.at[short(u)], y_pair)

    def y_rows(ylo_, k_):
        return pl.ds(pl.multiple_of(ylo_ * (2 * basis) + k_ * basis, 8), basis)

    def part_cols(u):
        at = c * width + u * pair + k * w
        return pl.ds(pl.multiple_of(at, 128), w)

    def c_copy(u):
        return remote(
            yr.at[u, y_rows(ylo, 1 - k)], out.at[:, part_cols(u)],
            sent.at[long(u)], c_recv.at[short(u)], sibling,
        )

    def h_copy(k_, u):
        return remote(
            yr.at[u, y_rows(1 - ylo, k_)], out.at[:, part_cols(u)],
            sent.at[long(u)], h_recv.at[short(u)], h_pair[k_],
        )

    def block_of(yhi_, x_, u):
        at = (yhi_ * 4 + x_) * width + u * pair
        return out.at[:, pl.ds(pl.multiple_of(at, 128), pair)]

    def h_landed(u):
        block = block_of(1 - yhi, x, u)
        return remote(block, block, sent.at[long(u)], h_recv.at[short(u)], sibling)

    x_plan = [
        (yhi, x, 0), (yhi, x, 1), (yhi, wrap(x - 1), 0),
        (1 - yhi, x, 0), (1 - yhi, x, 1), (1 - yhi, wrap(x + 1), 1),
    ]

    def x_copy(m, u):
        yhi_, x_, d = x_plan[m]
        block = block_of(yhi_, x_, u)
        recv = {0: x_recv.at[0, short(u)], 4: x_recv.at[1, short(u)]}.get(m, x_rest.at[long(u)])
        return remote(block, block, sent.at[long(u)], recv, x_next[d])

    def amount(strips):
        return out.at[:, pl.ds(0, strips * w)]

    def retired(u):
        return pltpu.make_async_copy(amount(31), amount(31), sent.at[long(u)])

    def rest_landed(u):
        return pltpu.make_async_copy(amount(8), amount(8), x_rest.at[long(u)])

    q_mine = pltpu.make_async_copy(q_ref, qv, q_own)
    q_mine.start()

    @pl.loop(0, AHEAD)
    def _(u):
        a_local(u).start()

    at_home = c == j
    barrier = pltpu.get_barrier_semaphore()
    for device in [sibling, *z_next, y_pair, *h_pair, *x_next]:
        pl.semaphore_signal(barrier, inc=1, device_id=device, device_id_type=MESH)

    @pl.loop(0, 8)
    def _(q):
        @pl.when(jnp.logical_not(jnp.logical_and(at_home, q == j)))
        def _():
            pl.semaphore_signal(barrier, inc=1, device_id=(2 * q + k, j), device_id_type=MESH)

    q_mine.wait()
    pl.semaphore_wait(barrier, 16 - jnp.where(at_home, 1, 0))

    @pl.loop(0, 8)
    def _(n):
        t = lax.rem(yhi + lax.rem(n, 2), 2) * 4 + lax.rem(x + 6 - lax.div(n, 2), 4)
        home = jnp.logical_and(at_home, t == c)

        @pl.when(jnp.logical_not(home))
        def _():
            q_push(t).start()

        @pl.when(home)
        def _():
            q_here().start()

    @pl.loop(0, 4)
    def _(u):
        a_swap(u).start()

    @pl.loop(0, 8)
    def _(q):
        q_landed(q).wait_recv()
        q_forward(q).start()

    @pl.loop(4, AHEAD)
    def _(u):
        a_swap(u).start()

    q_amount(8, f_recv).wait()
    high, low = halves(qf[...])
    qhi[...] = high
    qlo[...] = low

    def compute(d, u):
        a_local(u).wait()
        a_swap(u).wait_recv()
        a_high, a_low = halves(ab[u])
        p[u] = dot(qhi[...], a_low) + dot(qlo[...], a_high) + dot(qhi[...], a_high)

    def z_first(d, u):
        z_copy(2, d, u).start()
        z_copy(0, d, u).start()

    def fetch(d, u):
        @pl.when(u >= LONG)
        def _():
            a_swap(u - LONG).wait_send()

        a_local(u).start()
        a_swap(u).start()

    def z_on(d, u):
        z_copy(0, d, u).wait_recv()
        at = z_rows(1 - 2 * d)
        p[u, at] = p[u, at] + zr[0, u]
        z_copy(1, d, u).start()

    def z_last(d, u):
        z_copy(1, d, u).wait_recv()
        z_copy(2, d, u).wait_recv()
        at = z_rows(0)
        p[u, at] = p[u, at] + (zr[1, u] + zr[2, u])
        y_copy(u).start()

    def y_last(d, u):
        y_copy(u).wait_recv()
        total = p[u, z_rows(0)] + yr[u]
        yr[u] = total
        c_copy(u).start()
        for k_ in range(2):
            h_copy(k_, u).start()
        out[:, part_cols(u)] = yr[u, y_rows(ylo, k)]

    def spread(d, u):
        c_copy(u).wait_recv()
        x_copy(0, u).start()
        x_copy(1, u).start()

    def spread_far(d, u):
        h_landed(u).wait_recv()
        x_copy(3, u).start()
        x_copy(4, u).start()

    def forward(m, first):
        def body(d, u):
            x_copy(first, u).wait_recv()
            x_copy(m, u).start()
        return body

    def retire(d, u):
        rest_landed(u).wait()
        retired(u).wait()

    bodies = {
        "retire": retire, "fetch": fetch, "z2": z_last, "z1": z_on, "z0": z_first,
        "compute": compute, "y": y_last, "spread": spread, "far": spread_far,
        "near_on": forward(2, 0), "far_on": forward(5, 4),
    }
    lags = dict(STAGES)
    for u in range(-min(lags["compute"], lags["z0"])):
        for name in ("compute", "z0"):
            if u < -lags[name]:
                bodies[name](u % 2, u)

    @pl.loop(0, (units + max(lags.values()) + 1) // 2)
    def _(i):
        for d in range(2):
            for name, lag in STAGES:
                u = 2 * i + d - lag

                @pl.when(jnp.logical_and(u >= max(-lag, 0), u < units))
                def _():
                    bodies[name]((d - lag) % 2, u)

    @pl.loop(units - LONG, units)
    def _(u):
        a_swap(u).wait_send()

    q_amount(8, f_send).wait()

    @pl.when(at_home)
    def _():
        q_amount(7, q_send).wait()

    @pl.when(jnp.logical_not(at_home))
    def _():
        q_amount(8, q_send).wait()


def per_device(units, matrix, range_basis):
    rows, width = matrix.shape
    depth, basis = range_basis.shape
    w = width // units // 2
    dma = pltpu.SemaphoreType.DMA
    short, long = dma((SHORT,)), dma((LONG,))
    return pl.pallas_call(
        functools.partial(kernel, units),
        out_shape=pltpu.VMEM((basis, 8 * width), F32),
        in_specs=[pl.BlockSpec(memory_space=pl.ANY)] * 2,
        out_specs=pl.BlockSpec(memory_space=pltpu.VMEM),
        scratch_shapes=[
            pltpu.VMEM((units, 2 * rows, w), F32),
            pltpu.VMEM((basis, depth), F32),
            pltpu.VMEM((16 * basis, depth), F32),
            pltpu.VMEM((16 * basis, depth), BF16),
            pltpu.VMEM((16 * basis, depth), BF16),
            pltpu.VMEM((units, 16 * basis, w), F32),
            pltpu.VMEM((3, units, 4 * basis, w), F32),
            pltpu.VMEM((units, 4 * basis, w), F32),
            short, long, long, dma, dma, dma((8,)), dma, dma,
            long, dma((3, SHORT)), short, short, short, dma((2, SHORT)), long,
        ],
        compiler_params=pltpu.CompilerParams(
            collective_id=0, has_side_effects=True, vmem_limit_bytes=46 * 1024 * 1024
        ),
    )(matrix, range_basis.T)


def solution(mesh):
    in_specs = (P("row", "col"), P("col", "row"))
    out_specs = P("row", None)
    return jax.shard_map(
        functools.partial(per_device, UNITS), mesh=mesh, in_specs=in_specs, out_specs=out_specs, check_vma=False
    )
```

```python
import functools

import jax
import jax.numpy as jnp
from jax import lax
from jax.experimental import pallas as pl
from jax.experimental.pallas import tpu as pltpu
from jax.sharding import PartitionSpec as P

MESH = pl.DeviceIdType.MESH
UNITS = 64
SHORT, LONG = 10, 16
AHEAD = 6
F32 = jnp.float32
BF16 = jnp.bfloat16
STAGES = (
    ("spread", 7), ("far_on", 11), ("z1", 1), ("y", 6), ("compute", -2), ("z0", -2), ("far", 8), ("near_on", 9),
    ("z2", 3), ("retire", 13), ("fetch", -AHEAD),
)


def halves(value):
    high = value.astype(BF16)
    return high, (value - high.astype(F32)).astype(BF16)


def dot(left, right):
    return jnp.dot(left, right, preferred_element_type=F32)


def kernel(
    units, a_ref, q_ref, out,
    ab, qv, qf, qhi, qlo, p, zr, yr,
    a_own, a_send, a_recv, q_own, q_send, q_recv, f_send, f_recv,
    sent, z_recv, y_recv, c_recv, h_recv, x_recv, x_rest,
):
    rows, width = a_ref.shape
    basis = q_ref.shape[0]
    pair = width // units
    w = pair // 2

    r, c = lax.axis_index("row"), lax.axis_index("col")
    k = lax.rem(r, 2)
    j = lax.div(r, 2)
    z = lax.rem(j, 4)
    ylo = lax.div(j, 4)
    x = lax.rem(c, 4)
    yhi = lax.div(c, 4)

    def row_of(ylo_, z_, k_):
        return (ylo_ * 4 + z_) * 2 + k_

    def wrap(v):
        return lax.rem(v + 8, 4)

    sibling = (row_of(ylo, z, 1 - k), c)
    z_next = [(row_of(ylo, wrap(z + 1), k), c), (row_of(ylo, wrap(z - 1), k), c)]
    y_pair = (row_of(1 - ylo, z, k), c)
    h_pair = [(row_of(1 - ylo, z, k_), (1 - yhi) * 4 + x) for k_ in range(2)]
    x_next = [(r, yhi * 4 + wrap(x + 1)), (r, yhi * 4 + wrap(x - 1))]

    def remote(src, dst, send, recv, device):
        return pltpu.make_async_remote_copy(
            src_ref=src, dst_ref=dst, send_sem=send, recv_sem=recv,
            device_id=device, device_id_type=MESH,
        )

    def short(u):
        return lax.rem(u, SHORT)

    def long(u):
        return lax.rem(u, LONG)

    def a_local(u):
        cols = pl.ds(pl.multiple_of(u * pair + k * w, 128), w)
        at = pl.ds(pl.multiple_of(k * rows, 8), rows)
        return pltpu.make_async_copy(a_ref.at[:, cols], ab.at[u, at], a_own.at[short(u)])

    def a_swap(u):
        cols = pl.ds(pl.multiple_of(u * pair + (1 - k) * w, 128), w)
        at = pl.ds(pl.multiple_of(k * rows, 8), rows)
        return remote(a_ref.at[:, cols], ab.at[u, at], a_send, a_recv.at[long(u)], sibling)

    def q_rows(q, k_):
        at = lax.rem(q, 4) * (4 * basis) + lax.div(q, 4) * (2 * basis) + k_ * basis
        return pl.ds(pl.multiple_of(at, 8), basis)

    def q_push(t):
        return remote(qv, qf.at[q_rows(j, k)], q_send, q_recv.at[j], (c * 2 + k, t))

    def q_here():
        return pltpu.make_async_copy(q_ref, qf.at[q_rows(j, k)], q_recv.at[j])

    def q_landed(q):
        return remote(qv, qf.at[q_rows(q, k)], q_send, q_recv.at[q], sibling)

    def q_forward(q):
        block = qf.at[q_rows(q, k)]
        return remote(block, block, f_send, f_recv, sibling)

    def q_amount(blocks, sem):
        part = qf.at[pl.ds(0, blocks * basis)]
        return pltpu.make_async_copy(part, part, sem)

    def z_rows(away):
        return pl.ds(pl.multiple_of(wrap(z + away) * (4 * basis), 8), 4 * basis)

    def z_copy(kind, d, u):
        ahead = 1 - 2 * d
        away, way = ((2 * ahead, d), (ahead, d), (-ahead, 1 - d))[kind]
        return remote(
            p.at[u, z_rows(away)], zr.at[kind, u], sent.at[long(u)], z_recv.at[kind, short(u)], z_next[way]
        )

    def y_copy(u):
        return remote(p.at[u, z_rows(0)], yr.at[u], sent.at[long(u)], y_recv.at[short(u)], y_pair)

    def y_rows(ylo_, k_):
        return pl.ds(pl.multiple_of(ylo_ * (2 * basis) + k_ * basis, 8), basis)

    def part_cols(u):
        at = c * width + u * pair + k * w
        return pl.ds(pl.multiple_of(at, 128), w)

    def c_copy(u):
        return remote(
            yr.at[u, y_rows(ylo, 1 - k)], out.at[:, part_cols(u)],
            sent.at[long(u)], c_recv.at[short(u)], sibling,
        )

    def h_copy(k_, u):
        return remote(
            yr.at[u, y_rows(1 - ylo, k_)], out.at[:, part_cols(u)],
            sent.at[long(u)], h_recv.at[short(u)], h_pair[k_],
        )

    def block_of(yhi_, x_, u):
        at = (yhi_ * 4 + x_) * width + u * pair
        return out.at[:, pl.ds(pl.multiple_of(at, 128), pair)]

    def h_landed(u):
        block = block_of(1 - yhi, x, u)
        return remote(block, block, sent.at[long(u)], h_recv.at[short(u)], sibling)

    x_plan = [
        (yhi, x, 0), (yhi, x, 1), (yhi, wrap(x - 1), 0),
        (1 - yhi, x, 0), (1 - yhi, x, 1), (1 - yhi, wrap(x + 1), 1),
    ]

    def x_copy(m, u):
        yhi_, x_, d = x_plan[m]
        block = block_of(yhi_, x_, u)
        recv = {0: x_recv.at[0, short(u)], 4: x_recv.at[1, short(u)]}.get(m, x_rest.at[long(u)])
        return remote(block, block, sent.at[long(u)], recv, x_next[d])

    def amount(strips):
        return out.at[:, pl.ds(0, strips * w)]

    def retired(u):
        return pltpu.make_async_copy(amount(31), amount(31), sent.at[long(u)])

    def rest_landed(u):
        return pltpu.make_async_copy(amount(8), amount(8), x_rest.at[long(u)])

    at_home = c == j
    barrier = pltpu.get_barrier_semaphore()
    @pl.loop(0, 8)
    def _(q):
        @pl.when(jnp.logical_not(jnp.logical_and(at_home, q == j)))
        def _():
            pl.semaphore_signal(barrier, inc=1, device_id=(2 * q + k, j), device_id_type=MESH)

    for device in [sibling, *z_next, y_pair, *h_pair, *x_next]:
        pl.semaphore_signal(barrier, inc=1, device_id=device, device_id_type=MESH)

    q_mine = pltpu.make_async_copy(q_ref, qv, q_own)
    q_mine.start()

    @pl.loop(0, AHEAD)
    def _(u):
        a_local(u).start()

    q_mine.wait()
    pl.semaphore_wait(barrier, 16 - jnp.where(at_home, 1, 0))

    @pl.loop(0, 8)
    def _(n):
        t = lax.rem(yhi + 1 + lax.div(n, 4), 2) * 4 + lax.rem(x + 6 - lax.rem(n, 4), 4)
        home = jnp.logical_and(at_home, t == c)

        @pl.when(jnp.logical_not(home))
        def _():
            q_push(t).start()

        @pl.when(home)
        def _():
            q_here().start()

    @pl.loop(0, 4)
    def _(u):
        a_swap(u).start()

    @pl.loop(0, 8)
    def _(q):
        q_landed(q).wait_recv()
        q_forward(q).start()

    @pl.loop(4, AHEAD)
    def _(u):
        a_swap(u).start()

    q_amount(8, f_recv).wait()
    high, low = halves(qf[...])
    qhi[...] = high
    qlo[...] = low

    def compute(d, u):
        a_local(u).wait()
        a_swap(u).wait_recv()
        a_high, a_low = halves(ab[u])
        p[u] = dot(qhi[...], a_low) + dot(qlo[...], a_high) + dot(qhi[...], a_high)

    def z_first(d, u):
        z_copy(2, d, u).start()
        z_copy(0, d, u).start()

    def fetch(d, u):
        a_local(u).start()
        a_swap(u).start()

    def z_on(d, u):
        z_copy(0, d, u).wait_recv()
        at = z_rows(1 - 2 * d)
        p[u, at] = p[u, at] + zr[0, u]
        z_copy(1, d, u).start()

    def z_last(d, u):
        z_copy(1, d, u).wait_recv()
        z_copy(2, d, u).wait_recv()
        at = z_rows(0)
        p[u, at] = p[u, at] + (zr[1, u] + zr[2, u])
        y_copy(u).start()

    def y_last(d, u):
        y_copy(u).wait_recv()
        total = p[u, z_rows(0)] + yr[u]
        yr[u] = total
        c_copy(u).start()
        for k_ in range(2):
            h_copy(k_, u).start()
        out[:, part_cols(u)] = yr[u, y_rows(ylo, k)]

    def spread(d, u):
        c_copy(u).wait_recv()
        x_copy(0, u).start()
        x_copy(1, u).start()

    def spread_far(d, u):
        h_landed(u).wait_recv()
        x_copy(3, u).start()
        x_copy(4, u).start()

    def forward(m, first):
        def body(d, u):
            x_copy(first, u).wait_recv()
            x_copy(m, u).start()
        return body

    def retire(d, u):
        rest_landed(u).wait()
        retired(u).wait()

    bodies = {
        "retire": retire, "fetch": fetch, "z2": z_last, "z1": z_on, "z0": z_first,
        "compute": compute, "y": y_last, "spread": spread, "far": spread_far,
        "near_on": forward(2, 0), "far_on": forward(5, 4),
    }
    lags = dict(STAGES)
    for u in range(-min(lags["compute"], lags["z0"])):
        for name in ("compute", "z0"):
            if u < -lags[name]:
                bodies[name](u % 2, u)

    @pl.loop(0, (units + max(lags.values()) + 1) // 2)
    def _(i):
        for d in range(2):
            for name, lag in STAGES:
                u = 2 * i + d - lag

                @pl.when(jnp.logical_and(u >= max(-lag, 0), u < units))
                def _():
                    bodies[name]((d - lag) % 2, u)

    swapped = ab.at[pl.ds(0, units // 2)]
    pltpu.make_async_copy(swapped, swapped, a_send).wait()

    q_amount(8, f_send).wait()

    @pl.when(at_home)
    def _():
        q_amount(7, q_send).wait()

    @pl.when(jnp.logical_not(at_home))
    def _():
        q_amount(8, q_send).wait()


def per_device(units, matrix, range_basis):
    rows, width = matrix.shape
    depth, basis = range_basis.shape
    w = width // units // 2
    dma = pltpu.SemaphoreType.DMA
    short, long = dma((SHORT,)), dma((LONG,))
    return pl.pallas_call(
        functools.partial(kernel, units),
        out_shape=pltpu.VMEM((basis, 8 * width), F32),
        in_specs=[pl.BlockSpec(memory_space=pl.ANY)] * 2,
        out_specs=pl.BlockSpec(memory_space=pltpu.VMEM),
        scratch_shapes=[
            pltpu.VMEM((units, 2 * rows, w), F32),
            pltpu.VMEM((basis, depth), F32),
            pltpu.VMEM((16 * basis, depth), F32),
            pltpu.VMEM((16 * basis, depth), BF16),
            pltpu.VMEM((16 * basis, depth), BF16),
            pltpu.VMEM((units, 16 * basis, w), F32),
            pltpu.VMEM((3, units, 4 * basis, w), F32),
            pltpu.VMEM((units, 4 * basis, w), F32),
            short, dma, long, dma, dma, dma((8,)), dma, dma,
            long, dma((3, SHORT)), short, short, short, dma((2, SHORT)), long,
        ],
        compiler_params=pltpu.CompilerParams(
            collective_id=0, has_side_effects=True, vmem_limit_bytes=46 * 1024 * 1024
        ),
    )(matrix, range_basis.T)


def solution(mesh):
    in_specs = (P("row", "col"), P("col", "row"))
    out_specs = P("row", None)
    return jax.shard_map(
        functools.partial(per_device, UNITS), mesh=mesh, in_specs=in_specs, out_specs=out_specs, check_vma=False
    )
```

```python
import functools

import jax
import jax.numpy as jnp
from jax import lax
from jax.experimental import pallas as pl
from jax.experimental.pallas import tpu as pltpu
from jax.sharding import PartitionSpec as P

MESH = pl.DeviceIdType.MESH
UNITS = 64
SHORT, LONG = 10, 16
AHEAD = 6
F32 = jnp.float32
BF16 = jnp.bfloat16
STAGES = (
    ("z1", 1),
    ("spread", 7),
    ("compute", -2),
    ("z0", -2),
    ("far_on", 11),
    ("y", 6),
    ("far", 8),
    ("near_on", 9),
    ("z2", 3),
    ("retire", 13),
    ("fetch", -AHEAD),
)


def halves(value):
    high = value.astype(BF16)
    return high, (value - high.astype(F32)).astype(BF16)


def dot(left, right):
    return jnp.dot(left, right, preferred_element_type=F32)


def kernel(
    units, a_ref, q_ref, out,
    ab, qv, qf, qhi, qlo, p, zr, yr,
    a_own, a_send, a_recv, q_own, q_send, q_recv, f_send, f_recv,
    sent, z_recv, y_recv, c_recv, h_recv, x_recv, x_rest,
):
    rows, width = a_ref.shape
    basis = q_ref.shape[0]
    pair = width // units
    w = pair // 2

    r, c = lax.axis_index("row"), lax.axis_index("col")
    k = lax.rem(r, 2)
    j = lax.div(r, 2)
    z = lax.rem(j, 4)
    ylo = lax.div(j, 4)
    x = lax.rem(c, 4)
    yhi = lax.div(c, 4)

    def row_of(ylo_, z_, k_):
        return (ylo_ * 4 + z_) * 2 + k_

    def wrap(v):
        return lax.rem(v + 8, 4)

    sibling = (row_of(ylo, z, 1 - k), c)
    z_next = [(row_of(ylo, wrap(z + 1), k), c), (row_of(ylo, wrap(z - 1), k), c)]
    y_pair = (row_of(1 - ylo, z, k), c)
    h_pair = [(row_of(1 - ylo, z, k_), (1 - yhi) * 4 + x) for k_ in range(2)]
    x_next = [(r, yhi * 4 + wrap(x + 1)), (r, yhi * 4 + wrap(x - 1))]

    def remote(src, dst, send, recv, device):
        return pltpu.make_async_remote_copy(
            src_ref=src, dst_ref=dst, send_sem=send, recv_sem=recv,
            device_id=device, device_id_type=MESH,
        )

    def short(u):
        return lax.rem(u, SHORT)

    def long(u):
        return lax.rem(u, LONG)

    def a_local(u):
        cols = pl.ds(pl.multiple_of(u * pair + k * w, 128), w)
        at = pl.ds(pl.multiple_of(k * rows, 8), rows)
        return pltpu.make_async_copy(a_ref.at[:, cols], ab.at[u, at], a_own.at[short(u)])

    def a_swap(u):
        cols = pl.ds(pl.multiple_of(u * pair + (1 - k) * w, 128), w)
        at = pl.ds(pl.multiple_of(k * rows, 8), rows)
        return remote(a_ref.at[:, cols], ab.at[u, at], a_send, a_recv.at[long(u)], sibling)

    def q_rows(q, k_):
        at = lax.rem(q, 4) * (4 * basis) + lax.div(q, 4) * (2 * basis) + k_ * basis
        return pl.ds(pl.multiple_of(at, 8), basis)

    def q_push(t):
        return remote(qv, qf.at[q_rows(j, k)], q_send, q_recv.at[j], (c * 2 + k, t))

    def q_here():
        return pltpu.make_async_copy(q_ref, qf.at[q_rows(j, k)], q_recv.at[j])

    def q_landed(q):
        return remote(qv, qf.at[q_rows(q, k)], q_send, q_recv.at[q], sibling)

    def q_forward(q):
        block = qf.at[q_rows(q, k)]
        return remote(block, block, f_send, f_recv, sibling)

    def q_amount(blocks, sem):
        part = qf.at[pl.ds(0, blocks * basis)]
        return pltpu.make_async_copy(part, part, sem)

    def z_rows(away):
        return pl.ds(pl.multiple_of(wrap(z + away) * (4 * basis), 8), 4 * basis)

    def z_copy(kind, d, u):
        ahead = 1 - 2 * d
        away, way = ((2 * ahead, d), (ahead, d), (-ahead, 1 - d))[kind]
        return remote(
            p.at[u, z_rows(away)], zr.at[kind, u], sent.at[long(u)], z_recv.at[kind, short(u)], z_next[way]
        )

    def y_copy(u):
        return remote(p.at[u, z_rows(0)], yr.at[u], sent.at[long(u)], y_recv.at[short(u)], y_pair)

    def y_rows(ylo_, k_):
        return pl.ds(pl.multiple_of(ylo_ * (2 * basis) + k_ * basis, 8), basis)

    def part_cols(u):
        at = c * width + u * pair + k * w
        return pl.ds(pl.multiple_of(at, 128), w)

    def c_copy(u):
        return remote(
            yr.at[u, y_rows(ylo, 1 - k)], out.at[:, part_cols(u)],
            sent.at[long(u)], c_recv.at[short(u)], sibling,
        )

    def h_copy(k_, u):
        return remote(
            yr.at[u, y_rows(1 - ylo, k_)], out.at[:, part_cols(u)],
            sent.at[long(u)], h_recv.at[short(u)], h_pair[k_],
        )

    def block_of(yhi_, x_, u):
        at = (yhi_ * 4 + x_) * width + u * pair
        return out.at[:, pl.ds(pl.multiple_of(at, 128), pair)]

    def h_landed(u):
        block = block_of(1 - yhi, x, u)
        return remote(block, block, sent.at[long(u)], h_recv.at[short(u)], sibling)

    x_plan = [
        (yhi, x, 0), (yhi, x, 1), (yhi, wrap(x - 1), 0),
        (1 - yhi, x, 0), (1 - yhi, x, 1), (1 - yhi, wrap(x + 1), 1),
    ]

    def x_copy(m, u):
        yhi_, x_, d = x_plan[m]
        block = block_of(yhi_, x_, u)
        recv = {0: x_recv.at[0, short(u)], 4: x_recv.at[1, short(u)]}.get(m, x_rest.at[long(u)])
        return remote(block, block, sent.at[long(u)], recv, x_next[d])

    def amount(strips):
        return out.at[:, pl.ds(0, strips * w)]

    def retired(u):
        return pltpu.make_async_copy(amount(31), amount(31), sent.at[long(u)])

    def rest_landed(u):
        return pltpu.make_async_copy(amount(8), amount(8), x_rest.at[long(u)])

    at_home = c == j
    barrier = pltpu.get_barrier_semaphore()
    @pl.loop(0, 8)
    def _(q):
        @pl.when(jnp.logical_not(jnp.logical_and(at_home, q == j)))
        def _():
            pl.semaphore_signal(barrier, inc=1, device_id=(2 * q + k, j), device_id_type=MESH)

    for device in [sibling, *z_next, y_pair, *h_pair, *x_next]:
        pl.semaphore_signal(barrier, inc=1, device_id=device, device_id_type=MESH)

    q_mine = pltpu.make_async_copy(q_ref, qv, q_own)
    q_mine.start()

    @pl.loop(0, AHEAD)
    def _(u):
        a_local(u).start()

    q_mine.wait()
    pl.semaphore_wait(barrier, 16 - jnp.where(at_home, 1, 0))

    @pl.loop(0, 8)
    def _(n):
        t = lax.rem(yhi + 1 + lax.div(n, 4), 2) * 4 + lax.rem(x + 6 - lax.rem(n, 4), 4)
        home = jnp.logical_and(at_home, t == c)

        @pl.when(jnp.logical_not(home))
        def _():
            q_push(t).start()

        @pl.when(home)
        def _():
            q_here().start()

    @pl.loop(0, 4)
    def _(u):
        a_swap(u).start()

    @pl.loop(0, 8)
    def _(q):
        q_landed(q).wait_recv()
        q_forward(q).start()

    @pl.loop(4, AHEAD)
    def _(u):
        a_swap(u).start()

    q_amount(8, f_recv).wait()
    high, low = halves(qf[...])
    qhi[...] = high
    qlo[...] = low

    def compute(d, u):
        a_local(u).wait()
        a_swap(u).wait_recv()
        a_high, a_low = halves(ab[u])
        p[u] = dot(qhi[...], a_low) + dot(qlo[...], a_high) + dot(qhi[...], a_high)

    def z_first(d, u):
        z_copy(2, d, u).start()
        z_copy(0, d, u).start()

    def fetch(d, u):
        a_local(u).start()
        a_swap(u).start()

    def z_on(d, u):
        z_copy(0, d, u).wait_recv()
        at = z_rows(1 - 2 * d)
        p[u, at] = p[u, at] + zr[0, u]
        z_copy(1, d, u).start()

    def z_last(d, u):
        z_copy(1, d, u).wait_recv()
        z_copy(2, d, u).wait_recv()
        at = z_rows(0)
        p[u, at] = p[u, at] + (zr[1, u] + zr[2, u])
        y_copy(u).start()

    def y_last(d, u):
        y_copy(u).wait_recv()
        total = p[u, z_rows(0)] + yr[u]
        yr[u] = total
        c_copy(u).start()
        for k_ in range(2):
            h_copy(k_, u).start()
        out[:, part_cols(u)] = yr[u, y_rows(ylo, k)]

    def spread(d, u):
        c_copy(u).wait_recv()
        x_copy(0, u).start()
        x_copy(1, u).start()

    def spread_far(d, u):
        h_landed(u).wait_recv()
        x_copy(3, u).start()
        x_copy(4, u).start()

    def forward(m, first):
        def body(d, u):
            x_copy(first, u).wait_recv()
            x_copy(m, u).start()
        return body

    def retire(d, u):
        rest_landed(u).wait()
        retired(u).wait()

    bodies = {
        "retire": retire, "fetch": fetch, "z2": z_last, "z1": z_on, "z0": z_first,
        "compute": compute, "y": y_last, "spread": spread, "far": spread_far,
        "near_on": forward(2, 0), "far_on": forward(5, 4),
    }
    lags = dict(STAGES)
    for u in range(-min(lags["compute"], lags["z0"])):
        for name in ("compute", "z0"):
            if u < -lags[name]:
                bodies[name](u % 2, u)

    @pl.loop(0, (units + max(lags.values()) + 1) // 2)
    def _(i):
        for d in range(2):
            for name, lag in STAGES:
                u = 2 * i + d - lag

                @pl.when(jnp.logical_and(u >= max(-lag, 0), u < units))
                def _():
                    bodies[name]((d - lag) % 2, u)

    swapped = ab.at[pl.ds(0, units // 2)]
    pltpu.make_async_copy(swapped, swapped, a_send).wait()

    q_amount(8, f_send).wait()

    @pl.when(at_home)
    def _():
        q_amount(7, q_send).wait()

    @pl.when(jnp.logical_not(at_home))
    def _():
        q_amount(8, q_send).wait()


def per_device(units, matrix, range_basis):
    rows, width = matrix.shape
    depth, basis = range_basis.shape
    w = width // units // 2
    dma = pltpu.SemaphoreType.DMA
    short, long = dma((SHORT,)), dma((LONG,))
    return pl.pallas_call(
        functools.partial(kernel, units),
        out_shape=pltpu.VMEM((basis, 8 * width), F32),
        in_specs=[pl.BlockSpec(memory_space=pl.ANY)] * 2,
        out_specs=pl.BlockSpec(memory_space=pltpu.VMEM),
        scratch_shapes=[
            pltpu.VMEM((units, 2 * rows, w), F32),
            pltpu.VMEM((basis, depth), F32),
            pltpu.VMEM((16 * basis, depth), F32),
            pltpu.VMEM((16 * basis, depth), BF16),
            pltpu.VMEM((16 * basis, depth), BF16),
            pltpu.VMEM((units, 16 * basis, w), F32),
            pltpu.VMEM((3, units, 4 * basis, w), F32),
            pltpu.VMEM((units, 4 * basis, w), F32),
            short, dma, long, dma, dma, dma((8,)), dma, dma,
            long, dma((3, SHORT)), short, short, short, dma((2, SHORT)), long,
        ],
        compiler_params=pltpu.CompilerParams(
            collective_id=0, has_side_effects=True, vmem_limit_bytes=46 * 1024 * 1024
        ),
    )(matrix, range_basis.T)


def solution(mesh):
    in_specs = (P("row", "col"), P("col", "row"))
    out_specs = P("row", None)
    return jax.shard_map(
        functools.partial(per_device, UNITS), mesh=mesh, in_specs=in_specs, out_specs=out_specs, check_vma=False
    )
```
